32 devices in a mesh: row: 8 (over z, x), col: 4 (over y, core).
Axes of the slice: x: 2, y: 2, z: 4, core: 2. Of those that a mesh axis runs over, the one named last changes fastest.
Arguments:
- acquired_tiles: bfloat16 [4, 32768, 1024], P(None, ('row', 'col')), may hold values from -24 to 24
- row_live: int32 [4, 32768], P(None, ('row', 'col')), may hold values from 0 to 1, as said below
- col_live: int32 [4, 32768], P(None, ('row', 'col')), may hold values 0 or 1
- row_order: int32 [8], replicated, may hold values from 0 to 7, as said below
- source_init: float32 [32768, 256], P(('row', 'col')), may hold values from -3 to 3
- receiver_init: float32 [32768, 256], P(('row', 'col')), may hold values from -3 to 3
Outputs:
- sources: float32 [32768, 256], P(('row', 'col'))
- receivers: float32 [32768, 256], P(('row', 'col'))
The draws below stay inside these ranges and needn't reach their ends.
Inputs may be any that keep to these rules, and one draw needn't show every extreme that they name: `row_live`: 1 where the source of that row is recorded in that stratum's tile; sources go missing singly and in whole aligned lines of 128 rows, and the share of missing lines differs from block to block. `row_order`: each number once.
All inputs are finite; a program needn't handle non-finite values. No bound on the sum of `col_live` on one device may be relied on, other than what follows from the above.
Results may differ from the reference program's by a relative error of at most 0.00096.
Values sent between devices are 32-bit elements; how exact they have to be, the bound alone decides.
A program may use at most 128 MiB of HBM per device.

```python
import jax
import jax.numpy as jnp
from jax import lax

K = 256
BLOCK = 1024
BAND = 128
STRATA = 4
STEPS = 2
ORDER = 32768
N_ROW = 8
N_COL = 4
DEVICES = 32


def draw_row_live(key, part):
    seeded = jax.random.fold_in(key, 7)
    first_key, second_key = jax.random.split(seeded)
    band_total = ORDER // BAND
    owner_block = jnp.arange(band_total, dtype=jnp.int32) * BAND // BLOCK
    threshold = owner_block * 7 // DEVICES
    band_draw = jax.random.randint(first_key, (STRATA, band_total), 0, 10)
    band_live = (band_draw >= threshold[None, :]).astype(jnp.int32)
    single = (jax.random.randint(second_key, (STRATA, ORDER), 0, 5) > 0).astype(jnp.int32)
    return jnp.repeat(band_live, BAND, axis=1) * single


def draw_row_order(key, part):
    seeded = jax.random.fold_in(key, 17)
    perm_key, pick_key = jax.random.split(seeded)
    shuffled = jax.random.permutation(perm_key, N_ROW).astype(jnp.int32)
    chosen = jax.random.randint(pick_key, (), 0, N_ROW).astype(jnp.int32)
    wanted = (chosen + N_ROW - 1) % N_ROW
    positions = jnp.arange(N_ROW, dtype=jnp.int32)
    holder = jnp.sum(jnp.where(shuffled == wanted, positions, 0)).astype(jnp.int32)
    displaced = jnp.sum(jnp.where(positions == chosen, shuffled, 0)).astype(jnp.int32)
    result = jnp.where(positions == holder, displaced, shuffled)
    result = jnp.where(positions == chosen, wanted, result)
    return result.astype(jnp.int32)


def factor_draw(key, salt):
    seeded = jax.random.fold_in(key, salt)
    base_key = jax.random.fold_in(seeded, 0)
    values = 0.5 * jax.random.normal(base_key, (ORDER, K), jnp.float32)
    return jnp.clip(values, -3.0, 3.0)


def draw_source_init(key, part):
    return factor_draw(key, 11)


def draw_receiver_init(key, part):
    return factor_draw(key, 13)


def place_ends(drawn, rng, low, largest):
    index_at = [jax.random.randint(jax.random.fold_in(rng, axis), (), 0, length) for axis, length in enumerate(drawn.shape)]
    widest = drawn.shape.index(max(drawn.shape))
    neighbour = index_at[:widest] + [(index_at[widest] + 1) % drawn.shape[widest]] + index_at[widest + 1:]
    return drawn.at[tuple(index_at)].set(low).at[tuple(neighbour)].set(largest)


def steps_of(key, extent, pieces, smallest, top_value):
    loudness, own = 1.0, jax.random.fold_in(key, 6)
    for dim, parts in pieces:
        draws = jnp.exp(jax.random.uniform(jax.random.fold_in(own, dim), (parts,), jnp.float32, smallest / len(pieces), top_value / len(pieces)))
        loudness = loudness * jnp.repeat(draws, extent[dim] // parts).reshape([-1 if axis == dim else 1 for axis in range(len(extent))])
    return loudness


def scatter_about(own_key, shape, width, most, cuts=(), kind=jnp.bfloat16):
    level = steps_of(own_key, shape, cuts, -0.22, 0.18) if cuts else 1.0
    entries = jax.random.normal(own_key, shape, jnp.float32) * width * level
    return jnp.minimum(jnp.maximum(entries, -most), most).astype(kind)


def setup_inputs(seed: int = 0) -> dict:
    key_list = jax.random.split(jax.random.key(seed), 7)
    return {
        "acquired_tiles": scatter_about(key_list[0], (STRATA, ORDER, BLOCK), 4.0, 24.0, ((1, 32),)),
        "row_live": draw_row_live(jax.random.fold_in(key_list[6], 71), 0),
        "col_live": place_ends((jax.random.randint(key_list[2], (STRATA, ORDER), 0, 4) < 3).astype(jnp.int32), jax.random.fold_in(key_list[2], 1), 0, 1),
        "row_order": draw_row_order(jax.random.fold_in(key_list[6], 71), 0),
        "source_init": draw_source_init(jax.random.fold_in(key_list[6], 71), 0),
        "receiver_init": draw_receiver_init(jax.random.fold_in(key_list[6], 71), 0),
    }


def fit_block(src_block, rec_block, acquired, live_rows, live_cols):
    weights = live_rows.astype(jnp.float32)[:, None] * live_cols.astype(jnp.float32)[None, :]
    observed = acquired.astype(jnp.float32)
    step_size = 1.0 / (BLOCK + 2 * K)
    for iteration in range(STEPS):
        src_half = src_block.astype(jnp.bfloat16)
        rec_half = rec_block.astype(jnp.bfloat16)
        predicted = jnp.dot(src_half, rec_half.T, preferred_element_type=jnp.float32)
        misfit = (weights * (observed - predicted)).astype(jnp.bfloat16)
        grad_src = jnp.dot(misfit, rec_half, preferred_element_type=jnp.float32)
        grad_rec = jnp.dot(misfit.T, src_half, preferred_element_type=jnp.float32)
        src_block = src_block + step_size * grad_src
        rec_block = rec_block + step_size * grad_rec
    return src_block, rec_block


def reference(acquired_tiles, row_live, col_live, row_order, source_init, receiver_init):
    block_count = ORDER // BLOCK
    src_blocks = source_init.reshape(block_count, BLOCK, K)
    rec_blocks = receiver_init.reshape(block_count, BLOCK, K)
    for stratum in range(STRATA):
        slab_data = acquired_tiles[stratum].reshape(block_count, BLOCK, BLOCK)
        live_rows = row_live[stratum].reshape(block_count, BLOCK)
        live_cols = col_live[stratum].reshape(block_count, BLOCK)
        src_blocks, rec_blocks = lax.map(lambda packed: fit_block(*packed), (src_blocks, rec_blocks, slab_data, live_rows, live_cols))
        if stratum + 1 < STRATA:
            rec_blocks = jnp.roll(rec_blocks, 1, axis=0)
            if stratum == 1:
                rec_blocks = rec_blocks.reshape(N_ROW, N_COL, BLOCK, K)[row_order].reshape(block_count, BLOCK, K)
    return src_blocks.reshape(ORDER, K), rec_blocks.reshape(ORDER, K)
```

```python
import functools

import jax
import jax.numpy as jnp
from jax import lax
from jax.experimental import pallas as pl
from jax.experimental.pallas import tpu as pltpu
from jax.sharding import PartitionSpec as P

STEPS = 2
MESH = pl.DeviceIdType.MESH
F32 = jnp.float32
BF16 = jnp.bfloat16


def kernel(nr, nc, tiles, row_live, col_live, order, src_in, rec_in, src_out, rec_out,
           tile, rb, mid, out2, grad, half, half_t, row_mask,
           in_sem, ring_send, ring_recv, a_send, a_recv, b_send, b_recv):
    strata, block, width = tile.shape
    rank = src_out.shape[1]
    chunk = rb.shape[2]
    chunks = width // chunk
    piece = mid.shape[1]
    per_chunk = nr // chunks
    step_size = 1.0 / (width + 2 * rank)
    r = lax.axis_index("row")
    c = lax.axis_index("col")
    cn = lax.rem(c + 1, nc)
    rn = lax.rem(r + (c + 1) // nc, nr)
    cp = lax.rem(c + nc - 1, nc)

    loads = [
        pltpu.make_async_copy(tiles.at[s], tile.at[s], in_sem.at[s]) for s in range(strata)
    ]
    for load in loads:
        load.start()

    barrier = pltpu.get_barrier_semaphore()
    for k in range(nr):
        pl.semaphore_signal(barrier, inc=1, device_id={"row": k, "col": cp}, device_id_type=MESH)
    for k in range(1, nr):
        pl.semaphore_signal(
            barrier, inc=1, device_id={"row": lax.rem(r + k, nr), "col": c}, device_id_type=MESH
        )

    src_out[...] = src_in[...]
    for q in range(chunks):
        rb[0, q * rank:(q + 1) * rank, :] = rec_in[q * chunk:(q + 1) * chunk, :].T

    def ring_copy(s, q):
        lane = 0 if s == 0 else 1
        rows = pl.ds(q * rank, rank)
        return pltpu.make_async_remote_copy(
            src_ref=rb.at[s, rows], dst_ref=rb.at[s + 1, rows],
            send_sem=ring_send.at[lane, q], recv_sem=ring_recv.at[lane, q],
            device_id={"row": rn, "col": cn}, device_id_type=MESH,
        )

    def a_copy(s, p, slot):
        return pltpu.make_async_remote_copy(
            src_ref=rb.at[s, pl.ds(p * piece, piece)], dst_ref=mid.at[slot],
            send_sem=a_send.at[p], recv_sem=a_recv.at[slot],
            device_id={"row": p, "col": cn}, device_id_type=MESH,
        )

    def b_copy(s, to, p):
        return pltpu.make_async_remote_copy(
            src_ref=out2.at[to], dst_ref=rb.at[s + 1, pl.ds(p * piece, piece)],
            send_sem=b_send.at[to], recv_sem=b_recv.at[p],
            device_id={"row": to, "col": c}, device_id_type=MESH,
        )

    for s in range(strata):
        lanes = row_live[s:s + 1, :].astype(F32)
        for t in range(block // 128):
            row_mask[t * 128:(t + 1) * 128, :] = jnp.broadcast_to(
                lanes[:, t * 128:(t + 1) * 128], (128, 128)
            ).T * step_size
        loads[s].wait()
        for it in range(STEPS):
            half[...] = src_out[...].astype(BF16)
            half_t[...] = (src_out[...].T * lanes).astype(BF16)

            def one(q, carry, s=s, it=it):
                rows = pl.ds(pl.multiple_of(q * rank, rank), rank)
                cols = pl.ds(pl.multiple_of(q * chunk, chunk), chunk)
                if it == 0 and s > 0:
                    if s == 2:
                        for j in range(per_chunk):
                            p = q * per_chunk + j

                            @pl.when(p != r)
                            def _():
                                b_copy(1, r, p).wait_recv()
                    else:
                        ring_copy(s - 1, q).wait_recv()
                rec = rb[s, rows, :]
                rec_half = rec.astype(BF16)
                live = col_live[s:s + 1, cols].astype(F32)
                predicted = jnp.dot(half[...], rec_half, preferred_element_type=F32)
                misfit = (tile[s, :, cols].astype(F32) - predicted).astype(BF16)
                grad_rec = jnp.dot(half_t[...], misfit, preferred_element_type=F32)
                rb[s, rows, :] = rec + (step_size * live) * grad_rec
                grad_src = lax.dot_general(
                    misfit, (rec_half * live.astype(BF16)), (((1,), (1,)), ((), ())),
                    preferred_element_type=F32,
                )

                @pl.when(q == 0)
                def _():
                    grad[...] = grad_src

                @pl.when(q > 0)
                def _():
                    grad[...] += grad_src

                if it == STEPS - 1 and s in (0, 2):
                    ring_copy(s, q).start()
                return carry

            if s == 0 and it == 0:
                pass
            if it == STEPS - 1 and s == 0:
                pl.semaphore_wait(barrier, 2 * nr - 1)
            lax.fori_loop(0, chunks, one, 0)
            if it == STEPS - 1 and s == 1:
                def send_a(k, carry):
                    p = lax.rem(r + k, nr)
                    a_copy(1, p, rn).start()
                    return carry
                lax.fori_loop(0, nr, send_a, 0)
            for h in range(rank // 128):
                part = slice(h * 128, (h + 1) * 128)
                src_out[:, part] = src_out[:, part] + row_mask[...] * grad[:, part]
        if s == 1:
            def wait_a(k, carry):
                a_copy(1, 0, k).wait_recv()
                return carry
            lax.fori_loop(0, nr, wait_a, 0)
            rb[2, pl.ds(pl.multiple_of(r * piece, piece), piece), :] = mid[order[r]]

            def pick(k, carry):
                to = lax.rem(r + k, nr)
                out2[to] = mid[order[to]]
                return carry
            lax.fori_loop(1, nr, pick, 0)

            def send_b(k, carry):
                b_copy(1, lax.rem(r + k, nr), r).start()
                return carry
            lax.fori_loop(1, nr, send_b, 0)

    for q in range(chunks):
        rec_out[q * chunk:(q + 1) * chunk, :] = rb[strata - 1, q * rank:(q + 1) * rank, :].T
    for s in (0, 2):
        for q in range(chunks):
            ring_copy(s, q).wait_send()

    def done_a(k, carry):
        a_copy(1, k, 0).wait_send()
        return carry
    lax.fori_loop(0, nr, done_a, 0)

    def done_b(k, carry):
        b_copy(1, lax.rem(r + k, nr), r).wait_send()
        return carry
    lax.fori_loop(1, nr, done_b, 0)


def local(nr, nc, tiles, row_live, col_live, row_order, source_init, receiver_init):
    strata, block, width = tiles.shape
    rank = source_init.shape[1]
    chunk = width // 4
    chunks = width // chunk
    piece = chunks * rank // nr
    vmem = pl.BlockSpec(memory_space=pltpu.VMEM)
    return pl.pallas_call(
        functools.partial(kernel, nr, nc),
        out_shape=(
            jax.ShapeDtypeStruct(source_init.shape, F32),
            jax.ShapeDtypeStruct(receiver_init.shape, F32),
        ),
        in_specs=[
            pl.BlockSpec(memory_space=pl.ANY), vmem, vmem,
            pl.BlockSpec(memory_space=pltpu.SMEM), vmem, vmem,
        ],
        out_specs=(vmem, vmem),
        scratch_shapes=[
            pltpu.VMEM((strata, block, width), BF16),
            pltpu.VMEM((strata, chunks * rank, chunk), F32),
            pltpu.VMEM((nr, piece, chunk), F32),
            pltpu.VMEM((nr, piece, chunk), F32),
            pltpu.VMEM((block, rank), F32),
            pltpu.VMEM((block, rank), BF16),
            pltpu.VMEM((rank, block), BF16),
            pltpu.VMEM((block, 128), F32),
            pltpu.SemaphoreType.DMA((strata,)),
            pltpu.SemaphoreType.DMA((2, chunks)),
            pltpu.SemaphoreType.DMA((2, chunks)),
            pltpu.SemaphoreType.DMA((nr,)),
            pltpu.SemaphoreType.DMA((nr,)),
            pltpu.SemaphoreType.DMA((nr,)),
            pltpu.SemaphoreType.DMA((nr,)),
        ],
        compiler_params=pltpu.CompilerParams(
            collective_id=0, has_side_effects=True, vmem_limit_bytes=56 * 1024 * 1024
        ),
    )(tiles, row_live, col_live, row_order, source_init, receiver_init)


def solution(mesh):
    placed = (
        P(None, ("row", "col"), None),
        P(None, ("row", "col")),
        P(None, ("row", "col")),
        P(),
        P(("row", "col"), None),
        P(("row", "col"), None),
    )
    return jax.shard_map(
        functools.partial(local, mesh.shape["row"], mesh.shape["col"]),
        mesh=mesh,
        in_specs=placed,
        out_specs=(P(("row", "col"), None), P(("row", "col"), None)),
        check_vma=False,
    )
```
